128 devices in a mesh: enc: 4 (over z_lo, core), fsdp: 32 (over z_hi, x, y).
Axes of the slice: x: 4, y: 4, z: 4 (z_hi: 2, z_lo: 2; z = z_hi * 2 + z_lo), core: 2. Of those that a mesh axis runs over, the one named last changes fastest.
Arguments:
- enc_features: bfloat16 [32, 8, 1024, 512], P(None, 'enc', 'fsdp'), may hold values from -6 to 6
- enc_gain: float32 [1, 512], replicated, may hold values from 0.1 to 1.9
- enc_kernel: bfloat16 [1, 3, 512, 512], replicated, may hold values from -0.15625 to 0.15625
- out_kernel: bfloat16 [512, 16], replicated, may hold values from -0.25 to 0.25
- clip_start: int32 [32], replicated, may hold values from 0 to 3
- assign: int32 [32], replicated, may hold values from 0 to 31, each once
- embed_weight: bfloat16 [3072, 64], P('fsdp'), may hold values from -0.75 to 0.75
- mod_shift: float32 [32, 3072], P('fsdp'), may hold values from -3 to 3
- mod_scale: float32 [32, 3072], P('fsdp'), may hold values from -3 to 3
- value_weight: bfloat16 [3072, 1536], P('fsdp'), may hold values from -0.109375 to 0.109375
- value_cotangent: bfloat16 [32, 8, 256, 1536], P('fsdp', 'enc'), may hold values from -6 to 6
Outputs:
- values: bfloat16 [32, 8, 256, 1536], P('fsdp', 'enc')
- grad_value: float32 [3072, 1536], P(('enc', 'fsdp'))
- grad_embed: float32 [3072, 64], P(('enc', 'fsdp'))
The draws below stay inside these ranges and needn't reach their ends.
Inputs may be any that keep to these rules, and one draw needn't show every extreme that they name: Sample s is made from clip assign[s]; every clip is taken by exactly one sample.
All inputs are finite; a program needn't handle non-finite values.
Results may differ from the reference program's by a relative error of at most 0.025.
Values may be sent and summed in bfloat16 or wider, within the bound.
No kernel may reach another device: no remote copies, remote signals or barrier semaphores. Data moves between devices by JAX's collectives and lax.ppermute only.
A program may use at most 192 MiB of HBM per device.

```python
import jax
import jax.numpy as jnp
from jax import lax

D = 3072
C = 512
LAT = 16
L_ENC = 1
CLIPS = 32
FRAMES = 8
PATCHES = 256
PIX = 1024
HALF = 1536


def with_ends(values, own_key, least, high):
    longest = values.shape.index(max(values.shape))
    spots = []
    for shift in (0, 1):
        where = [jax.random.randint(jax.random.fold_in(own_key, axis), (), 0, length) for axis, length in enumerate(values.shape)]
        where[longest] = (where[longest] + shift) % values.shape[longest]
        spots.append(tuple(where))
    return values.at[spots[0]].set(least).at[spots[1]].set(high)


def block_scale(rng, extent, cuts, least, high):
    def one(dim, shards_of):
        draws = jax.random.uniform(jax.random.fold_in(jax.random.fold_in(rng, 6), dim), (shards_of,), jnp.float32, least / len(cuts), high / len(cuts))
        return jnp.repeat(jnp.exp(draws), extent[dim] // shards_of).reshape((-1,) + (1,) * (len(extent) - dim - 1))

    level = one(*cuts[0])
    for cut in cuts[1:]:
        level = level * one(*cut)
    return level


def gaussian(own_key, extent, width, limit, shards=(), kind=jnp.bfloat16):
    entries = jax.random.normal(own_key, extent, jnp.float32) * width
    if len(shards) > 0:
        entries = block_scale(own_key, extent, shards, -0.22, 0.18) * entries
    return jnp.clip(entries, min=-limit, max=limit).astype(kind)


def setup_inputs(seed: int = 0) -> dict:
    seeds = jax.random.split(jax.random.key(seed), 12)
    return {
        "enc_features": gaussian(seeds[0], (CLIPS, FRAMES, PIX, C), 1.0, 6.0, ((1, 4), (2, 32))),
        "enc_gain": jnp.clip(1.0 + 0.18 * jax.random.normal(seeds[1], (L_ENC, C), jnp.float32), 0.1, 1.9),
        "enc_kernel": gaussian(seeds[2], (L_ENC, 3, C, C), (3 * C) ** -0.5, 0.15625),
        "out_kernel": gaussian(seeds[3], (C, LAT), C ** -0.5, 0.25),
        "clip_start": with_ends(jax.random.randint(seeds[4], (CLIPS,), 0, FRAMES // 2), jax.random.fold_in(seeds[4], 1), 0, (FRAMES // 2) - 1).astype(jnp.int32),
        "assign": jax.random.permutation(seeds[5], CLIPS).astype(jnp.int32),
        "embed_weight": gaussian(seeds[6], (D, 4 * LAT), (4 * LAT) ** -0.5, 0.75, ((0, 32),)),
        "mod_shift": gaussian(seeds[7], (CLIPS, D), 0.5, 3.0, ((0, 32),), jnp.float32),
        "mod_scale": gaussian(seeds[8], (CLIPS, D), 0.5, 3.0, ((0, 32),), jnp.float32),
        "value_weight": gaussian(seeds[9], (D, HALF), D ** -0.5, 0.109375, ((0, 32),)),
        "value_cotangent": gaussian(seeds[10], (CLIPS, FRAMES, PATCHES, HALF), 1.0, 6.0, ((0, 32), (1, 4))),
    }


def encode_clip(features, start_frame, enc_gain, enc_kernel, out_kernel):
    frame_count = features.shape[0]
    live_mask = (jnp.arange(frame_count, dtype=jnp.int32) >= start_frame).astype(jnp.float32)[:, None, None]
    stored = features
    for layer_index in range(L_ENC):
        activation = stored.astype(jnp.float32)
        scaling = lax.rsqrt(lax.optimization_barrier(jnp.mean(activation * activation, axis=-1, keepdims=True)) + 1e-06)
        normed = (live_mask * activation * scaling * enc_gain[layer_index]).astype(jnp.bfloat16)
        padded = jnp.concatenate([jnp.zeros((2,) + normed.shape[1:], jnp.bfloat16), normed], axis=0)
        convolved = jnp.zeros(activation.shape, jnp.float32)
        for offset in range(3):
            window = padded[offset:offset + frame_count].reshape(-1, C)
            convolved = convolved + jnp.dot(window, enc_kernel[layer_index, offset], preferred_element_type=jnp.float32).reshape(activation.shape)
        stored = lax.optimization_barrier((activation + jax.nn.silu(convolved)).astype(jnp.bfloat16))
    latent = jnp.dot(stored.reshape(-1, C), out_kernel, preferred_element_type=jnp.float32).reshape(frame_count, PIX, LAT)
    latent = (latent * live_mask).astype(jnp.bfloat16)
    return latent.reshape(frame_count, PATCHES, 4 * LAT)

def reference(enc_features, enc_gain, enc_kernel, out_kernel, clip_start, assign, embed_weight, mod_shift, mod_scale, value_weight, value_cotangent):

    def encode_one(inputs_pair):
        return encode_clip(inputs_pair[0], inputs_pair[1], enc_gain, enc_kernel, out_kernel)
    latents = lax.map(encode_one, (enc_features, clip_start))
    samples = jnp.take(latents, assign.astype(jnp.int32), axis=0)

    def sample_step(carry, inputs_tuple):
        grad_w_sum, grad_e_sum = carry
        patch_block, shift_row, scale_row, cot_block = inputs_tuple
        token_rows = patch_block.reshape(-1, 4 * LAT)
        mixed = jnp.dot(token_rows, embed_weight.T, preferred_element_type=jnp.float32)
        row_mean = lax.optimization_barrier(jnp.mean(mixed, axis=-1, keepdims=True))
        centred = mixed - row_mean
        row_var = lax.optimization_barrier(jnp.mean(centred * centred, axis=-1, keepdims=True))
        inv_std = lax.rsqrt(row_var + 1e-06)
        unit = centred * inv_std
        modulated = (unit * (1.0 + scale_row) + shift_row).astype(jnp.bfloat16)
        projected = jnp.dot(modulated, value_weight, preferred_element_type=jnp.float32).astype(jnp.bfloat16)
        cot_rows = cot_block.reshape(-1, HALF)
        grad_w = jnp.dot(modulated.T, cot_rows, preferred_element_type=jnp.float32)
        grad_mod = jnp.dot(cot_rows, value_weight.T, preferred_element_type=jnp.float32)
        grad_unit = grad_mod * (1.0 + scale_row)
        grad_mixed = inv_std * (grad_unit - lax.optimization_barrier(jnp.mean(grad_unit, axis=-1, keepdims=True)) - unit * lax.optimization_barrier(jnp.mean(grad_unit * unit, axis=-1, keepdims=True)))
        grad_bf = grad_mixed.astype(jnp.bfloat16)
        grad_e = jnp.dot(grad_bf.T, token_rows, preferred_element_type=jnp.float32)
        return ((grad_w_sum + grad_w, grad_e_sum + grad_e), projected.reshape(cot_block.shape))
    start_carry = (jnp.zeros((D, HALF), jnp.float32), jnp.zeros((D, 4 * LAT), jnp.float32))
    (grad_value, grad_embed), values = lax.scan(sample_step, start_carry, (samples, mod_shift, mod_scale, value_cotangent))
    return (values, grad_value, grad_embed)
```

```python
import jax
import jax.numpy as jnp
from jax import lax
from jax.experimental import pallas as pl
from jax.experimental.pallas import tpu as pltpu
from jax.sharding import Mesh
from jax.sharding import PartitionSpec as P


BF = jnp.bfloat16
F32 = jnp.float32
AXES = ("zl", "c", "zh", "x", "y")
SIZES = (2, 2, 2, 4, 4)


def hop(values, dest):
    pairs = []
    for i in range(128):
        at, rest = {}, i
        for name, size in zip(reversed(AXES), reversed(SIZES)):
            at[name], rest = rest % size, rest // size
        to = {**at, **dest(at)}
        j = 0
        for name, size in zip(AXES, SIZES):
            j = j * size + to[name]
        pairs.append((i, j))
    return lax.ppermute(values, AXES, pairs)


def along(axis, by):
    def dest(at):
        if axis == "z":
            z = (at["zh"] * 2 + at["zl"] + by) % 4
            return {"zh": z // 2, "zl": z % 2}
        return {axis: (at[axis] + by) % 4}

    return dest


def by_core(first, second):
    return lambda at: (first if at["c"] == 0 else second)(at)


def swap(x, axis):
    return lax.ppermute(x, axis, [(0, 1), (1, 0)])


def pick(x, index, dim):
    return lax.dynamic_index_in_dim(x, index, dim, keepdims=False)


def place_kernel(idx, own, up, down, far, own2, up2, down2, far2, out, sems):
    c, a_at, b_at = idx[0], idx[1], idx[2]
    zh = idx[3]
    copies = []

    def put(pieces, a_first, b):
        for i in range(2):
            for j in range(2):
                a = a_first + i - 2 * i * (a_first % 2)
                z = zh + j - 2 * j * zh
                at_x = jnp.where(c == 0, a, b)
                at_y = jnp.where(c == 0, b, a)
                copies.append(
                    pltpu.make_async_copy(
                        pieces.at[i, j], out.at[z, at_x, at_y], sems.at[len(copies)]
                    )
                )

    for first, group in ((a_at, (own, up, down, far)), (3 - a_at, (own2, up2, down2, far2))):
        for pieces, back in zip(group, (0, 3, 1, 2)):
            put(pieces, first, (b_at + back) % 4)
    for copy in copies:
        copy.start()
    for copy in copies:
        copy.wait()


def nearest(at):
    z = 3 - (at["zh"] * 2 + at["zl"])
    return {"zh": z // 2, "zl": z % 2}


def place(idx, pieces, lanes):
    rows = pieces[0].shape[2]
    out = pl.pallas_call(
        place_kernel,
        out_shape=jax.ShapeDtypeStruct((2, 4, 4, rows, lanes), BF),
        in_specs=[pl.BlockSpec(memory_space=pltpu.SMEM)]
        + [pl.BlockSpec(memory_space=pltpu.HBM)] * 8,
        out_specs=pl.BlockSpec(memory_space=pltpu.VMEM),
        scratch_shapes=[pltpu.SemaphoreType.DMA((32,))],
        compiler_params=pltpu.CompilerParams(vmem_limit_bytes=24 << 20),
        cost_estimate=pl.CostEstimate(
            flops=0, transcendentals=0, bytes_accessed=128 * rows * lanes
        ),
        name="place",
    )(idx, *pieces)
    return out.reshape(32 * rows, lanes)


def conv_kernel(feat, before, normed, kernels, out_kernel, out):
    b, n = before[...], normed[...]
    channels = n.shape[-1]
    middle = jnp.concatenate([b[:, 1:], n[:, :1]], axis=1)
    total = None
    for k, window in enumerate((b, middle, n)):
        part = jnp.dot(
            window.reshape(-1, channels), kernels[k], preferred_element_type=F32
        )
        total = part if total is None else total + part
    activation = feat[...].astype(F32).reshape(total.shape)
    stored = (activation + total / (1.0 + jnp.exp(-total))).astype(BF)
    latent = jnp.dot(stored, out_kernel[...], preferred_element_type=F32)
    out[...] = latent.astype(BF).reshape(out.shape)


def conv_clips(features, first, before, normed, kernels, out_kernel):
    clips, frames, pixels, channels = normed.shape
    step, lat = 8, out_kernel.shape[1]
    block = pl.BlockSpec((step, frames, pixels, channels), lambda i: (i, 0, 0, 0))
    return pl.pallas_call(
        conv_kernel,
        grid=(clips // step,),
        out_shape=jax.ShapeDtypeStruct((clips, frames, pixels, lat), BF),
        in_specs=[
            pl.BlockSpec(
                (step, frames, pixels, channels), lambda i: (i + first // step, 0, 0, 0)
            ),
            block,
            block,
            pl.BlockSpec(kernels.shape, lambda i: (0, 0, 0)),
            pl.BlockSpec(out_kernel.shape, lambda i: (0, 0)),
        ],
        out_specs=pl.BlockSpec((step, frames, pixels, lat), lambda i: (i, 0, 0, 0)),
        compiler_params=pltpu.CompilerParams(
            dimension_semantics=("arbitrary",), vmem_limit_bytes=32 << 20
        ),
        cost_estimate=pl.CostEstimate(
            flops=clips * frames * pixels * channels * channels * 6,
            transcendentals=0,
            bytes_accessed=4 << 20,
        ),
        name="conv",
    )(features, before, normed, kernels, out_kernel)


def unit_of(tok, embed):
    mixed = lax.dot_general(
        tok, embed, (((1,), (1,)), ((), ())), preferred_element_type=F32
    )
    centred = mixed - jnp.mean(mixed, axis=-1, keepdims=True)
    inv_std = lax.rsqrt(jnp.mean(centred * centred, axis=-1, keepdims=True) + 1e-06)
    return centred * inv_std, inv_std


def forward_kernel(idx, tok, embed, scale, shift, out_all, out_kept, out_given):
    c = idx[0]
    unit, _ = unit_of(tok[...], embed[...])
    out_all[...] = (unit * (1.0 + scale[...]) + shift[...]).astype(BF)
    quarter = out_all.shape[1] // 4
    for zl in range(2):
        here = pl.ds(zl * quarter, quarter)
        at = pl.multiple_of((2 * zl + c) * quarter, 128)
        out_kept[:, here] = out_all[:, pl.ds(at, quarter)]
        at = pl.multiple_of((2 * zl + 1 - c) * quarter, 128)
        out_given[:, here] = out_all[:, pl.ds(at, quarter)]


def backward_kernel(
    idx, tok_t, tok, embed, scaling, cot_t, w_kept, w_got, out_e, grad_ref, mixed_ref, grad_bf, acc
):
    c, step = idx[0], pl.program_id(0)
    block, half = w_kept.shape
    width, lanes = grad_ref.shape
    group = 32

    def against(at, weight):
        at = pl.multiple_of(at * half, 128)
        return jnp.dot(weight[...], cot_t[pl.ds(at, half), :], preferred_element_type=F32)

    rows = pl.ds(pl.multiple_of(step * block, block), block)
    factor = jnp.concatenate([scaling[...]] * (lanes // scaling.shape[1]), axis=1)
    grad_ref[rows, :] = (against(c, w_kept) + against(1 - c, w_got)) * factor
    mixed_ref[rows, :] = jnp.dot(
        embed[...], tok_t[...], preferred_element_type=F32
    )

    @pl.when(step == 0)
    def _():
        acc[...] = jnp.zeros(acc.shape, F32)

    origin = mixed_ref[0:1, :]

    def load(first, i):
        here = pl.ds(pl.multiple_of(first + i * group, group), group)
        return here, mixed_ref[here, :] - origin, grad_ref[here, :]

    def fold(v):
        return jnp.sum(v.reshape(group // 8, 8, lanes), axis=0)

    def sums(i, carry):
        _, shifted, grad = load(step * block, i)
        for k, v in enumerate((shifted, shifted * shifted, grad, grad * shifted)):
            acc[k] += fold(v)
        return carry

    lax.fori_loop(0, block // group, sums, 0)

    @pl.when(step == pl.num_programs(0) - 1)
    def _():
        mean, square, mean_g, product = (
            jnp.sum(acc[k], axis=0, keepdims=True) * (1.0 / width) for k in range(4)
        )
        inv_std = lax.rsqrt(jnp.maximum(square - mean * mean, 0.0) + 1e-06)
        slope = (product - mean * mean_g) * inv_std * inv_std

        def finish(i, carry):
            here, shifted, grad = load(0, i)
            grad_bf[here, :] = (inv_std * (grad - mean_g - (shifted - mean) * slope)).astype(BF)
            return carry

        lax.fori_loop(0, width // group, finish, 0)
        out_e[...] = jnp.dot(grad_bf[...], tok[...], preferred_element_type=F32)


def backward_call(core, tok_t, tok, embed, scaling, cot_t, w_kept, w_got):
    width, tokens, block = embed.shape[0], tok.shape[0], 512

    def stays(a):
        return pl.BlockSpec(a.shape, lambda i, _: (0, 0))

    def by_rows(a):
        return pl.BlockSpec((block, a.shape[1]), lambda i, _: (i, 0))

    return pl.pallas_call(
        backward_kernel,
        grid_spec=pltpu.PrefetchScalarGridSpec(
            num_scalar_prefetch=1,
            grid=(width // block,),
            in_specs=[
                stays(tok_t),
                stays(tok),
                by_rows(embed),
                by_rows(scaling),
                stays(cot_t),
                by_rows(w_kept),
                by_rows(w_got),
            ],
            out_specs=pl.BlockSpec((width, tok.shape[1]), lambda i, _: (0, 0)),
            scratch_shapes=[
                pltpu.VMEM((width, tokens), F32),
                pltpu.VMEM((width, tokens), F32),
                pltpu.VMEM((width, tokens), BF),
                pltpu.VMEM((4, 8, tokens), F32),
            ],
        ),
        out_shape=jax.ShapeDtypeStruct((width, tok.shape[1]), F32),
        compiler_params=pltpu.CompilerParams(
            dimension_semantics=("arbitrary",), vmem_limit_bytes=40 << 20
        ),
        cost_estimate=pl.CostEstimate(
            flops=2 * tokens * width * cot_t.shape[0],
            transcendentals=0,
            bytes_accessed=16 << 20,
        ),
        name="backward",
    )(core, tok_t, tok, embed, scaling, cot_t, w_kept, w_got)


def values_kernel(idx, mod, weight, *rest):
    rest[-1][...] = jnp.dot(mod[...], weight[...], preferred_element_type=F32).astype(BF)


def values_call(side, mod, weight, before=None):
    tokens, width = mod.shape
    half, step = weight.shape[1], 256
    steps = half // step
    rest = [] if before is None else [before]
    return pl.pallas_call(
        values_kernel,
        grid_spec=pltpu.PrefetchScalarGridSpec(
            num_scalar_prefetch=1,
            grid=(steps,),
            in_specs=[
                pl.BlockSpec((tokens, width), lambda i, _: (0, 0)),
                pl.BlockSpec((width, step), lambda i, _: (0, i)),
            ]
            + [pl.BlockSpec(memory_space=pl.ANY)] * len(rest),
            out_specs=pl.BlockSpec((tokens, step), lambda i, idx: (0, idx[0] * steps + i)),
        ),
        out_shape=jax.ShapeDtypeStruct((tokens, 2 * half), BF),
        input_output_aliases={} if before is None else {3: 0},
        compiler_params=pltpu.CompilerParams(
            dimension_semantics=("arbitrary",), vmem_limit_bytes=32 << 20
        ),
        cost_estimate=pl.CostEstimate(
            flops=2 * tokens * width * half, transcendentals=0, bytes_accessed=7 << 20
        ),
        name="values",
    )(side, mod, weight, *rest)


def rows_call(kernel, idx, blocked, whole, outs, flops=0):
    tokens, step = blocked[0].shape[0], 256

    def by_rows(a):
        return pl.BlockSpec((step, a.shape[1]), lambda i, _: (i, 0))

    def stays(a):
        return pl.BlockSpec(a.shape, lambda i, _: (0, 0))

    return pl.pallas_call(
        kernel,
        grid_spec=pltpu.PrefetchScalarGridSpec(
            num_scalar_prefetch=1,
            grid=(tokens // step,),
            in_specs=[stays(a) if a_whole else by_rows(a) for a, a_whole in zip(blocked, whole)],
            out_specs=[by_rows(o) if o.shape[0] == tokens else stays(o) for o in outs],
        ),
        out_shape=outs,
        compiler_params=pltpu.CompilerParams(
            dimension_semantics=("arbitrary",), vmem_limit_bytes=48 << 20
        ),
        cost_estimate=pl.CostEstimate(flops=flops, transcendentals=0, bytes_accessed=16 << 20),
    )(idx, *blocked)


def exchange(latent, embed_weight, assign):
    clips, rows = latent.shape[0], embed_weight.shape[0]
    ordered = jnp.take(latent, assign, axis=0).reshape(clips, -1, 128)
    packed = jnp.concatenate([embed_weight[: rows // 2], embed_weight[rows // 2 :]], axis=1)
    packed = jnp.broadcast_to(packed, (clips,) + packed.shape)
    both = jnp.concatenate([packed, ordered], axis=1)
    both = lax.all_to_all(both, ("zh", "x", "y"), split_axis=0, concat_axis=0, tiled=True)
    embed = both[:, : rows // 2]
    embed = jnp.concatenate([embed[..., :64], embed[..., 64:]], axis=1).reshape(-1, 64)
    frames = latent.shape[1]
    tokens = both[:, rows // 2 :].reshape(clips, frames, -1, 64)
    return jnp.swapaxes(tokens, 0, 1).reshape(-1, 64), embed


def ring_reduce(part, cut, forward, back, beside=None):
    def halves(p):
        return p[:cut], p[cut:]

    far_a, far_b = halves(part(2))
    up_a, up_b = halves(part(1))
    down_a, down_b = halves(part(3))
    own_a, own_b = halves(part(0))
    send_f = jnp.concatenate([far_a, up_b], axis=0)
    send_b = jnp.concatenate([far_b, down_a], axis=0)
    got_f = hop(send_f, forward)
    got_b = hop(send_b, back)
    from_a, near_b = halves(got_f)
    from_b, near_a = halves(got_b)
    tied = lax.optimization_barrier
    one = None
    if beside is not None:
        one = beside((send_f, send_b))
        from_a, from_b, one = tied((from_a, from_b, one))
    sum_a = (up_a.astype(F32) + from_a.astype(F32)).astype(BF)
    sum_b = (down_b.astype(F32) + from_b.astype(F32)).astype(BF)
    last_a = hop(sum_a, forward)
    last_b = hop(sum_b, back)
    a = own_a.astype(F32) + near_a.astype(F32) + last_a.astype(F32)
    b = own_b.astype(F32) + near_b.astype(F32) + last_b.astype(F32)
    return jnp.concatenate([a, b], axis=0), one


def direct_reduce(part, dest):
    total = part(0).astype(F32)
    for d in (1, 3, 2):
        got = hop(part(d), dest(d))
        total = total + got.astype(F32)
    return total


def channel_norm(activation, gain_row):
    scaling = lax.rsqrt(jnp.mean(activation * activation, axis=-1, keepdims=True) + 1e-06)
    return activation * scaling * gain_row


def norm_clips(enc_features, enc_gain, clip_start):
    frame_count = enc_features.shape[1]
    enc_index = lax.axis_index("zl") * 2 + lax.axis_index("c")
    frame_ids = enc_index * frame_count + jnp.arange(frame_count, dtype=jnp.int32)
    live_mask = (frame_ids[None, :] >= clip_start[:, None]).astype(F32)[:, :, None, None]
    normed = live_mask * channel_norm(enc_features.astype(F32), enc_gain[0])
    return normed.astype(BF), live_mask


def as_patches(latent, live_mask):
    clips, frames, pixels, lat = latent.shape
    latent = latent * live_mask.astype(BF)
    return latent.reshape(clips, frames, pixels // 4, 4 * lat)


def local(
    enc_features,
    enc_gain,
    enc_kernel,
    out_kernel,
    clip_start,
    assign,
    embed_weight,
    mod_shift,
    mod_scale,
    value_weight,
    value_cotangent,
):
    pos = {name: lax.axis_index(name) for name in AXES}
    c = pos["c"]
    cols = value_cotangent.shape[-1]
    half = cols // 2
    cot_rows = value_cotangent.reshape(-1, cols)
    tokens = cot_rows.shape[0]
    tied = lax.optimization_barrier
    zh, x, y = pos["zh"], pos["x"], pos["y"]
    rows = value_weight.shape[0]
    own = lax.dynamic_slice_in_dim(value_weight, c * half, half, axis=1)
    a_at = jnp.where(c == 0, x, y)
    b_at = jnp.where(c == 0, y, x)
    got_z = hop(own, nearest)
    clips = enc_features.shape[0]

    def group(k, features):
        part = slice(k * clips // 2, (k + 1) * clips // 2)
        normed, live_mask = norm_clips(features[part], enc_gain, clip_start[part])
        before = lax.ppermute(normed, ("zl", "c"), [(0, 1), (1, 2), (2, 3)])
        return normed, before, live_mask

    def latents(k, normed, before, live_mask):
        latent = conv_clips(
            enc_features, k * clips // 2, before, normed, enc_kernel[0], out_kernel
        )
        return as_patches(latent, live_mask)

    group_a = group(0, enc_features)
    got_z, _ = tied((got_z, group_a[0]))
    pair = jnp.stack([own, got_z])
    one = hop(pair, by_core(lambda at: {"x": at["x"] ^ 1}, lambda at: {"y": at["y"] ^ 1}))
    features, _ = tied((enc_features, got_z))
    group_b = group(1, features)
    one, _ = tied((one, group_b[0]))
    other_cot = swap(cot_rows, "c")
    two = jnp.stack([pair, one])
    four = hop(two, by_core(lambda at: {"x": 3 - at["x"]}, lambda at: {"y": 3 - at["y"]}))
    ahead = by_core(along("y", 1), along("x", 1))
    behind = by_core(along("y", 3), along("x", 3))
    up = hop(two, ahead)
    down = hop(two, behind)

    latent_a = latents(0, *group_a)
    up2 = hop(four, ahead)
    down2 = hop(four, behind)
    far = hop(up, ahead)
    latent_b = latents(1, *group_b)
    token_rows, embed_full = exchange(jnp.concatenate([latent_a, latent_b]), embed_weight, assign)
    late_cot, late_scale, _ = tied((cot_rows, mod_scale, latent_b))
    cot_t = late_cot.T
    scaling = jnp.broadcast_to((1.0 + late_scale).reshape(-1, 1), (mod_scale.shape[1], 128))
    far2 = hop(down2, behind)
    idx = jnp.stack([c, a_at, b_at, zh]).astype(jnp.int32)
    pieces = (two, up, down, far, four, up2, down2, far2)
    width = embed_full.shape[0]
    quarter = width // 4
    core = jnp.reshape(c, (1,)).astype(jnp.int32)

    modulated, kept, given = rows_call(
        forward_kernel,
        core,
        (token_rows, embed_full, mod_scale, mod_shift),
        (False, True, True, True),
        [
            jax.ShapeDtypeStruct((tokens, width), BF),
            jax.ShapeDtypeStruct((tokens, width // 2), BF),
            jax.ShapeDtypeStruct((tokens, width // 2), BF),
        ],
        flops=2 * tokens * width * 512,
    )
    got = swap(given, "c")
    weight_kept = place(idx, pieces, half)
    weight_got = swap(weight_kept, "c")
    mod_rows = jnp.concatenate([kept, got], axis=0)
    cot_both = jnp.concatenate([cot_rows, other_cot], axis=0)
    grad_w = lax.dot_general(
        mod_rows, cot_both, (((0,), (0,)), ((), ())), preferred_element_type=F32
    ).astype(BF)
    blocks_w = grad_w.reshape(4, 4, 96, cols)

    def x_at(d):
        return (pos["x"] + d) % 4

    def z_at(d):
        z = (pos["zh"] * 2 + pos["zl"] + d) % 4
        return (z % 2) * 2 + z // 2

    def cut(blocks, d):
        return jnp.where(c == 0, pick(blocks, x_at(d), 1), pick(blocks, z_at(d), 0))

    projected = values_call(core, modulated, weight_kept)

    def embed_gradient(after):
        tok, _ = tied((token_rows, after))
        grad_e = backward_call(
            core, tok.T, tok, embed_full, scaling, cot_t, weight_kept, weight_got
        )
        grad_e = grad_e.reshape(2, 2, quarter, -1)
        given = swap(pick(grad_e, 1 - c, 1).astype(BF), "c")
        return grad_e, given

    projected = values_call(1 - core, modulated, weight_got, projected)

    forward = [by_core(along("x", 1), along("z", 1)), by_core(along("z", 1), along("x", 1))]
    back = [by_core(along("x", 3), along("z", 3)), by_core(along("z", 3), along("x", 3))]
    chunk, (grad_e, given_e) = ring_reduce(
        lambda d: cut(blocks_w, d), 2, forward[0], back[0], embed_gradient
    )
    grad_e = (pick(grad_e, c, 1) + given_e.astype(F32)).astype(BF).reshape(4, 4, 96, -1)
    chunk_e = direct_reduce(
        lambda d: cut(grad_e, d), lambda d: by_core(along("x", d), along("z", d))
    )
    chunk = jnp.concatenate([chunk.astype(BF), chunk_e.astype(BF)], axis=-1)

    def second(d):
        return pick(chunk, jnp.where(c == 0, z_at(d), x_at(d)), 0)

    rows, _ = ring_reduce(second, 48, forward[1], back[1])
    rows = rows.reshape(4, 24, -1)
    summed = direct_reduce(lambda d: pick(rows, (pos["y"] + d) % 4, 0), lambda d: along("y", d))
    grad_value = summed[:, :cols]
    grad_embed = summed[:, cols:]

    return (projected.reshape(value_cotangent.shape), grad_value, grad_embed)


def solution(mesh):
    sub = Mesh(mesh.devices.reshape(SIZES), AXES)
    enc, fsdp = ("zl", "c"), ("zh", "x", "y")
    in_specs = (
        P(None, enc, fsdp, None),
        P(),
        P(),
        P(),
        P(),
        P(),
        P(fsdp, None),
        P(fsdp, None),
        P(fsdp, None),
        P(fsdp, None),
        P(fsdp, enc, None, None),
    )
    out_specs = (P(fsdp, enc, None, None), P(enc + fsdp, None), P(enc + fsdp, None))
    return jax.shard_map(local, mesh=sub, in_specs=in_specs, out_specs=out_specs, check_vma=False)
```

```python
import jax
import jax.numpy as jnp
from jax import lax
from jax.experimental import pallas as pl
from jax.experimental.pallas import tpu as pltpu
from jax.sharding import Mesh
from jax.sharding import PartitionSpec as P


BF = jnp.bfloat16
F32 = jnp.float32
AXES = ("zl", "c", "zh", "x", "y")
SIZES = (2, 2, 2, 4, 4)


def hop(values, dest):
    pairs = []
    for i in range(128):
        at, rest = {}, i
        for name, size in zip(reversed(AXES), reversed(SIZES)):
            at[name], rest = rest % size, rest // size
        to = {**at, **dest(at)}
        j = 0
        for name, size in zip(AXES, SIZES):
            j = j * size + to[name]
        pairs.append((i, j))
    return lax.ppermute(values, AXES, pairs)


def along(axis, by):
    def dest(at):
        if axis == "z":
            z = (at["zh"] * 2 + at["zl"] + by) % 4
            return {"zh": z // 2, "zl": z % 2}
        return {axis: (at[axis] + by) % 4}

    return dest


def by_core(first, second):
    return lambda at: (first if at["c"] == 0 else second)(at)


def swap(x, axis):
    return lax.ppermute(x, axis, [(0, 1), (1, 0)])


def pick(x, index, dim):
    return lax.dynamic_index_in_dim(x, index, dim, keepdims=False)


def place_kernel(idx, own, up, down, far, own2, up2, down2, far2, out, sems):
    c, a_at, b_at = idx[0], idx[1], idx[2]
    zh = idx[3]
    copies = []

    def put(pieces, a_first, b):
        for i in range(2):
            for j in range(2):
                a = a_first + i - 2 * i * (a_first % 2)
                z = zh + j - 2 * j * zh
                at_x = jnp.where(c == 0, a, b)
                at_y = jnp.where(c == 0, b, a)
                copies.append(
                    pltpu.make_async_copy(
                        pieces.at[i, j], out.at[z, at_x, at_y], sems.at[len(copies)]
                    )
                )

    for first, group in ((a_at, (own, up, down, far)), (3 - a_at, (own2, up2, down2, far2))):
        for pieces, back in zip(group, (0, 3, 1, 2)):
            put(pieces, first, (b_at + back) % 4)
    for copy in copies:
        copy.start()
    for copy in copies:
        copy.wait()


def nearest(at):
    z = 3 - (at["zh"] * 2 + at["zl"])
    return {"zh": z // 2, "zl": z % 2}


def place(idx, pieces, lanes):
    rows = pieces[0].shape[2]
    out = pl.pallas_call(
        place_kernel,
        out_shape=jax.ShapeDtypeStruct((2, 4, 4, rows, lanes), BF),
        in_specs=[pl.BlockSpec(memory_space=pltpu.SMEM)]
        + [pl.BlockSpec(memory_space=pltpu.HBM)] * 8,
        out_specs=pl.BlockSpec(memory_space=pltpu.VMEM),
        scratch_shapes=[pltpu.SemaphoreType.DMA((32,))],
        compiler_params=pltpu.CompilerParams(vmem_limit_bytes=24 << 20),
        cost_estimate=pl.CostEstimate(
            flops=0, transcendentals=0, bytes_accessed=128 * rows * lanes
        ),
        name="place",
    )(idx, *pieces)
    return out.reshape(32 * rows, lanes)


def flip_kernel(x, out):
    out[...] = x[...].T


def flip(x):
    rows, cols = x.shape
    step = 384
    return pl.pallas_call(
        flip_kernel,
        grid=(cols // step,),
        out_shape=jax.ShapeDtypeStruct((cols, rows), x.dtype),
        in_specs=[pl.BlockSpec((rows, step), lambda i: (0, i))],
        out_specs=pl.BlockSpec((step, rows), lambda i: (i, 0)),
        cost_estimate=pl.CostEstimate(flops=0, transcendentals=0, bytes_accessed=4 * rows * cols),
        name="flip",
    )(x)


def conv_kernel(feat, before, normed, kernels, out_kernel, out):
    b, n = before[...], normed[...]
    channels = n.shape[-1]
    middle = jnp.concatenate([b[:, 1:], n[:, :1]], axis=1)
    total = None
    for k, window in enumerate((b, middle, n)):
        part = jnp.dot(
            window.reshape(-1, channels), kernels[k], preferred_element_type=F32
        )
        total = part if total is None else total + part
    activation = feat[...].astype(F32).reshape(total.shape)
    stored = (activation + total / (1.0 + jnp.exp(-total))).astype(BF)
    latent = jnp.dot(stored, out_kernel[...], preferred_element_type=F32)
    out[...] = latent.astype(BF).reshape(out.shape)


def conv_clips(features, first, before, normed, kernels, out_kernel):
    clips, frames, pixels, channels = normed.shape
    step, lat = 8, out_kernel.shape[1]
    block = pl.BlockSpec((step, frames, pixels, channels), lambda i: (i, 0, 0, 0))
    return pl.pallas_call(
        conv_kernel,
        grid=(clips // step,),
        out_shape=jax.ShapeDtypeStruct((clips, frames, pixels, lat), BF),
        in_specs=[
            pl.BlockSpec(
                (step, frames, pixels, channels), lambda i: (i + first // step, 0, 0, 0)
            ),
            block,
            block,
            pl.BlockSpec(kernels.shape, lambda i: (0, 0, 0)),
            pl.BlockSpec(out_kernel.shape, lambda i: (0, 0)),
        ],
        out_specs=pl.BlockSpec((step, frames, pixels, lat), lambda i: (i, 0, 0, 0)),
        compiler_params=pltpu.CompilerParams(
            dimension_semantics=("arbitrary",), vmem_limit_bytes=32 << 20
        ),
        cost_estimate=pl.CostEstimate(
            flops=clips * frames * pixels * channels * channels * 6,
            transcendentals=0,
            bytes_accessed=4 << 20,
        ),
        name="conv",
    )(features, before, normed, kernels, out_kernel)


def unit_of(tok, embed):
    mixed = lax.dot_general(
        tok, embed, (((1,), (1,)), ((), ())), preferred_element_type=F32
    )
    centred = mixed - jnp.mean(mixed, axis=-1, keepdims=True)
    inv_std = lax.rsqrt(jnp.mean(centred * centred, axis=-1, keepdims=True) + 1e-06)
    return centred * inv_std, inv_std


def forward_kernel(idx, tok, embed, scale, shift, out_all, out_kept, out_given):
    c = idx[0]
    unit, _ = unit_of(tok[...], embed[...])
    out_all[...] = (unit * (1.0 + scale[...]) + shift[...]).astype(BF)
    quarter = out_all.shape[1] // 4
    for zl in range(2):
        here = pl.ds(zl * quarter, quarter)
        at = pl.multiple_of((2 * zl + c) * quarter, 128)
        out_kept[:, here] = out_all[:, pl.ds(at, quarter)]
        at = pl.multiple_of((2 * zl + 1 - c) * quarter, 128)
        out_given[:, here] = out_all[:, pl.ds(at, quarter)]


def backward_kernel(
    idx, tok_t, tok, embed, scaling, cot_t, w_kept, w_got, out_e, grad_ref, mixed_ref, grad_bf, acc
):
    c, step = idx[0], pl.program_id(0)
    block, half = w_kept.shape
    width, lanes = grad_ref.shape
    group = 32

    def against(at, weight):
        at = pl.multiple_of(at * half, 128)
        return jnp.dot(weight[...], cot_t[pl.ds(at, half), :], preferred_element_type=F32)

    rows = pl.ds(pl.multiple_of(step * block, block), block)
    factor = jnp.concatenate([scaling[...]] * (lanes // scaling.shape[1]), axis=1)
    grad_ref[rows, :] = (against(c, w_kept) + against(1 - c, w_got)) * factor
    mixed_ref[rows, :] = jnp.dot(
        embed[...], tok_t[...], preferred_element_type=F32
    )

    @pl.when(step == 0)
    def _():
        acc[...] = jnp.zeros(acc.shape, F32)

    origin = mixed_ref[0:1, :]

    def load(first, i):
        here = pl.ds(pl.multiple_of(first + i * group, group), group)
        return here, mixed_ref[here, :] - origin, grad_ref[here, :]

    def fold(v):
        return jnp.sum(v.reshape(group // 8, 8, lanes), axis=0)

    def sums(i, carry):
        _, shifted, grad = load(step * block, i)
        for k, v in enumerate((shifted, shifted * shifted, grad, grad * shifted)):
            acc[k] += fold(v)
        return carry

    lax.fori_loop(0, block // group, sums, 0)

    @pl.when(step == pl.num_programs(0) - 1)
    def _():
        mean, square, mean_g, product = (
            jnp.sum(acc[k], axis=0, keepdims=True) * (1.0 / width) for k in range(4)
        )
        inv_std = lax.rsqrt(jnp.maximum(square - mean * mean, 0.0) + 1e-06)
        slope = (product - mean * mean_g) * inv_std * inv_std

        def finish(i, carry):
            here, shifted, grad = load(0, i)
            grad_bf[here, :] = (inv_std * (grad - mean_g - (shifted - mean) * slope)).astype(BF)
            return carry

        lax.fori_loop(0, width // group, finish, 0)
        out_e[...] = jnp.dot(grad_bf[...], tok[...], preferred_element_type=F32)


def backward_call(core, tok_t, tok, embed, scaling, cot_t, w_kept, w_got):
    width, tokens, block = embed.shape[0], tok.shape[0], 512

    def stays(a):
        return pl.BlockSpec(a.shape, lambda i, _: (0, 0))

    def by_rows(a):
        return pl.BlockSpec((block, a.shape[1]), lambda i, _: (i, 0))

    return pl.pallas_call(
        backward_kernel,
        grid_spec=pltpu.PrefetchScalarGridSpec(
            num_scalar_prefetch=1,
            grid=(width // block,),
            in_specs=[
                stays(tok_t),
                stays(tok),
                by_rows(embed),
                by_rows(scaling),
                stays(cot_t),
                by_rows(w_kept),
                by_rows(w_got),
            ],
            out_specs=pl.BlockSpec((width, tok.shape[1]), lambda i, _: (0, 0)),
            scratch_shapes=[
                pltpu.VMEM((width, tokens), F32),
                pltpu.VMEM((width, tokens), F32),
                pltpu.VMEM((width, tokens), BF),
                pltpu.VMEM((4, 8, tokens), F32),
            ],
        ),
        out_shape=jax.ShapeDtypeStruct((width, tok.shape[1]), F32),
        compiler_params=pltpu.CompilerParams(
            dimension_semantics=("arbitrary",), vmem_limit_bytes=40 << 20
        ),
        cost_estimate=pl.CostEstimate(
            flops=2 * tokens * width * cot_t.shape[0],
            transcendentals=0,
            bytes_accessed=16 << 20,
        ),
        name="backward",
    )(core, tok_t, tok, embed, scaling, cot_t, w_kept, w_got)


def values_kernel(idx, mod, weight, *rest):
    rest[-1][...] = jnp.dot(mod[...], weight[...], preferred_element_type=F32).astype(BF)


def values_call(side, mod, weight, before=None):
    tokens, width = mod.shape
    half, step = weight.shape[1], 256
    steps = half // step
    rest = [] if before is None else [before]
    return pl.pallas_call(
        values_kernel,
        grid_spec=pltpu.PrefetchScalarGridSpec(
            num_scalar_prefetch=1,
            grid=(steps,),
            in_specs=[
                pl.BlockSpec((tokens, width), lambda i, _: (0, 0)),
                pl.BlockSpec((width, step), lambda i, _: (0, i)),
            ]
            + [pl.BlockSpec(memory_space=pl.ANY)] * len(rest),
            out_specs=pl.BlockSpec((tokens, step), lambda i, idx: (0, idx[0] * steps + i)),
        ),
        out_shape=jax.ShapeDtypeStruct((tokens, 2 * half), BF),
        input_output_aliases={} if before is None else {3: 0},
        compiler_params=pltpu.CompilerParams(
            dimension_semantics=("arbitrary",), vmem_limit_bytes=32 << 20
        ),
        cost_estimate=pl.CostEstimate(
            flops=2 * tokens * width * half, transcendentals=0, bytes_accessed=7 << 20
        ),
        name="values",
    )(side, mod, weight, *rest)


def rows_call(kernel, idx, blocked, whole, outs, flops=0):
    tokens, step = blocked[0].shape[0], 256

    def by_rows(a):
        return pl.BlockSpec((step, a.shape[1]), lambda i, _: (i, 0))

    def stays(a):
        return pl.BlockSpec(a.shape, lambda i, _: (0, 0))

    return pl.pallas_call(
        kernel,
        grid_spec=pltpu.PrefetchScalarGridSpec(
            num_scalar_prefetch=1,
            grid=(tokens // step,),
            in_specs=[stays(a) if a_whole else by_rows(a) for a, a_whole in zip(blocked, whole)],
            out_specs=[by_rows(o) if o.shape[0] == tokens else stays(o) for o in outs],
        ),
        out_shape=outs,
        compiler_params=pltpu.CompilerParams(
            dimension_semantics=("arbitrary",), vmem_limit_bytes=48 << 20
        ),
        cost_estimate=pl.CostEstimate(flops=flops, transcendentals=0, bytes_accessed=16 << 20),
    )(idx, *blocked)


def exchange(latent, embed_weight, assign):
    clips, rows = latent.shape[0], embed_weight.shape[0]
    ordered = jnp.take(latent, assign, axis=0).reshape(clips, -1, 128)
    packed = jnp.concatenate([embed_weight[: rows // 2], embed_weight[rows // 2 :]], axis=1)
    packed = jnp.broadcast_to(packed, (clips,) + packed.shape)
    both = jnp.concatenate([packed, ordered], axis=1)
    both = lax.all_to_all(both, ("zh", "x", "y"), split_axis=0, concat_axis=0, tiled=True)
    embed = both[:, : rows // 2]
    embed = jnp.concatenate([embed[..., :64], embed[..., 64:]], axis=1).reshape(-1, 64)
    frames = latent.shape[1]
    tokens = both[:, rows // 2 :].reshape(clips, frames, -1, 64)
    return jnp.swapaxes(tokens, 0, 1).reshape(-1, 64), embed


def ring_reduce(part, cut, forward, back, beside=None):
    def halves(p):
        return p[:cut], p[cut:]

    far_a, far_b = halves(part(2))
    up_a, up_b = halves(part(1))
    down_a, down_b = halves(part(3))
    own_a, own_b = halves(part(0))
    send_f = jnp.concatenate([far_a, up_b], axis=0)
    send_b = jnp.concatenate([far_b, down_a], axis=0)
    got_f = hop(send_f, forward)
    got_b = hop(send_b, back)
    tied = lax.optimization_barrier
    one = None
    if beside is not None:
        one = beside((send_f, send_b))
        got_f, got_b, one = tied((got_f, got_b, one))
    from_a, near_b = halves(got_f)
    from_b, near_a = halves(got_b)
    sum_a = (up_a.astype(F32) + from_a.astype(F32)).astype(BF)
    sum_b = (down_b.astype(F32) + from_b.astype(F32)).astype(BF)
    last_a = hop(sum_a, forward)
    last_b = hop(sum_b, back)
    a = own_a.astype(F32) + near_a.astype(F32) + last_a.astype(F32)
    b = own_b.astype(F32) + near_b.astype(F32) + last_b.astype(F32)
    return jnp.concatenate([a, b], axis=0), one


def direct_reduce(part, dest):
    total = part(0).astype(F32)
    for d in (1, 3, 2):
        got = hop(part(d), dest(d))
        total = total + got.astype(F32)
    return total


def channel_norm(activation, gain_row):
    scaling = lax.rsqrt(jnp.mean(activation * activation, axis=-1, keepdims=True) + 1e-06)
    return activation * scaling * gain_row


def norm_clips(enc_features, enc_gain, clip_start):
    frame_count = enc_features.shape[1]
    enc_index = lax.axis_index("zl") * 2 + lax.axis_index("c")
    frame_ids = enc_index * frame_count + jnp.arange(frame_count, dtype=jnp.int32)
    live_mask = (frame_ids[None, :] >= clip_start[:, None]).astype(F32)[:, :, None, None]
    normed = live_mask * channel_norm(enc_features.astype(F32), enc_gain[0])
    return normed.astype(BF), live_mask


def as_patches(latent, live_mask):
    clips, frames, pixels, lat = latent.shape
    latent = latent * live_mask.astype(BF)
    return latent.reshape(clips, frames, pixels // 4, 4 * lat)


def local(
    enc_features,
    enc_gain,
    enc_kernel,
    out_kernel,
    clip_start,
    assign,
    embed_weight,
    mod_shift,
    mod_scale,
    value_weight,
    value_cotangent,
):
    pos = {name: lax.axis_index(name) for name in AXES}
    c = pos["c"]
    cols = value_cotangent.shape[-1]
    half = cols // 2
    cot_rows = value_cotangent.reshape(-1, cols)
    tokens = cot_rows.shape[0]
    tied = lax.optimization_barrier
    zh, x, y = pos["zh"], pos["x"], pos["y"]
    rows = value_weight.shape[0]
    own = lax.dynamic_slice_in_dim(value_weight, c * half, half, axis=1)
    a_at = jnp.where(c == 0, x, y)
    b_at = jnp.where(c == 0, y, x)
    got_z = hop(own, nearest)
    bounds = (0, 16, 32)
    kernels = pltpu.with_memory_space_constraint(enc_kernel[0], pltpu.HBM)

    def group(k, features):
        part = slice(*bounds[k : k + 2])
        normed, live_mask = norm_clips(features[part], enc_gain, clip_start[part])
        before = lax.ppermute(normed, ("zl", "c"), [(0, 1), (1, 2), (2, 3)])
        return normed, before, live_mask

    def latents(k, normed, before, live_mask):
        latent = conv_clips(
            enc_features, bounds[k], before, normed, kernels, out_kernel
        )
        return as_patches(latent, live_mask)

    group_a = group(0, enc_features)
    got_z, _ = tied((got_z, group_a[0]))
    pair = jnp.stack([own, got_z])
    one = hop(pair, by_core(lambda at: {"x": at["x"] ^ 1}, lambda at: {"y": at["y"] ^ 1}))
    features, _ = tied((enc_features, got_z))
    group_b = group(1, features)
    one, _ = tied((one, group_b[0]))
    other_cot = swap(cot_rows, "c")
    two = jnp.stack([pair, one])
    four = hop(two, by_core(lambda at: {"x": 3 - at["x"]}, lambda at: {"y": 3 - at["y"]}))
    ahead = by_core(along("y", 1), along("x", 1))
    behind = by_core(along("y", 3), along("x", 3))
    up = hop(two, ahead)
    down = hop(two, behind)

    latent_a = latents(0, *group_a)
    up2 = hop(four, ahead)
    down2 = hop(four, behind)
    far = hop(up, ahead)
    latent_b = latents(1, *group_b)
    token_rows, embed_full = exchange(jnp.concatenate([latent_a, latent_b]), embed_weight, assign)
    late_cot, late_scale, _ = tied((cot_rows, mod_scale, latent_b))
    cot_t = flip(late_cot)
    scaling = jnp.broadcast_to((1.0 + late_scale).reshape(-1, 1), (mod_scale.shape[1], 128))
    far2 = hop(down2, behind)
    idx = jnp.stack([c, a_at, b_at, zh]).astype(jnp.int32)
    pieces = (two, up, down, far, four, up2, down2, far2)
    width = embed_full.shape[0]
    quarter = width // 4
    core = jnp.reshape(c, (1,)).astype(jnp.int32)

    modulated, kept, given = rows_call(
        forward_kernel,
        core,
        (token_rows, embed_full, mod_scale, mod_shift),
        (False, True, True, True),
        [
            jax.ShapeDtypeStruct((tokens, width), BF),
            jax.ShapeDtypeStruct((tokens, width // 2), BF),
            jax.ShapeDtypeStruct((tokens, width // 2), BF),
        ],
        flops=2 * tokens * width * 512,
    )
    got = swap(given, "c")
    weight_kept = place(idx, pieces, half)
    weight_got = swap(weight_kept, "c")
    mod_rows = jnp.concatenate([kept, got], axis=0)
    cot_both = jnp.concatenate([cot_rows, other_cot], axis=0)
    grad_w = lax.dot_general(
        mod_rows, cot_both, (((0,), (0,)), ((), ())), preferred_element_type=F32
    ).astype(BF)
    blocks_w = grad_w.reshape(4, 4, 96, cols)

    def x_at(d):
        return (pos["x"] + d) % 4

    def z_at(d):
        z = (pos["zh"] * 2 + pos["zl"] + d) % 4
        return (z % 2) * 2 + z // 2

    def cut(blocks, d):
        return jnp.where(c == 0, pick(blocks, x_at(d), 1), pick(blocks, z_at(d), 0))

    projected = values_call(core, modulated, weight_kept)

    def embed_gradient(after):
        tok, _ = tied((token_rows, after))
        grad_e = backward_call(
            core, tok.T, tok, embed_full, scaling, cot_t, weight_kept, weight_got
        )
        grad_e = grad_e.reshape(2, 2, quarter, -1)
        given = swap(pick(grad_e, 1 - c, 1).astype(BF), "c")
        return grad_e, given

    projected = values_call(1 - core, modulated, weight_got, projected)

    forward = by_core(along("x", 1), along("z", 1))
    back = by_core(along("x", 3), along("z", 3))
    chunk, (grad_e, given_e) = ring_reduce(
        lambda d: cut(blocks_w, d), 2, forward, back, embed_gradient
    )
    grad_e = (pick(grad_e, c, 1) + given_e.astype(F32)).astype(BF).reshape(4, 4, 96, -1)
    chunk_e = direct_reduce(
        lambda d: cut(grad_e, d), lambda d: by_core(along("x", d), along("z", d))
    )
    chunk = jnp.concatenate([chunk.astype(BF), chunk_e.astype(BF)], axis=-1)

    def second(d):
        return pick(chunk, jnp.where(c == 0, z_at(d), x_at(d)), 0)

    rows = direct_reduce(second, lambda d: by_core(along("z", d), along("x", d)))
    rows = rows.reshape(4, 24, -1)
    summed = direct_reduce(lambda d: pick(rows, (pos["y"] + d) % 4, 0), lambda d: along("y", d))
    grad_value = summed[:, :cols]
    grad_embed = summed[:, cols:]

    return (projected.reshape(value_cotangent.shape), grad_value, grad_embed)


def solution(mesh):
    sub = Mesh(mesh.devices.reshape(SIZES), AXES)
    enc, fsdp = ("zl", "c"), ("zh", "x", "y")
    in_specs = (
        P(None, enc, fsdp, None),
        P(),
        P(),
        P(),
        P(),
        P(),
        P(fsdp, None),
        P(fsdp, None),
        P(fsdp, None),
        P(fsdp, None),
        P(fsdp, enc, None, None),
    )
    out_specs = (P(fsdp, enc, None, None), P(enc + fsdp, None), P(enc + fsdp, None))
    return jax.shard_map(local, mesh=sub, in_specs=in_specs, out_specs=out_specs, check_vma=False)
```

```python
import jax
import jax.numpy as jnp
from jax import lax
from jax.experimental import pallas as pl
from jax.experimental.pallas import tpu as pltpu
from jax.sharding import Mesh
from jax.sharding import PartitionSpec as P


BF = jnp.bfloat16
F32 = jnp.float32
AXES = ("zl", "c", "zh", "x", "y")
SIZES = (2, 2, 2, 4, 4)


def hop(values, dest):
    pairs = []
    for i in range(128):
        at, rest = {}, i
        for name, size in zip(reversed(AXES), reversed(SIZES)):
            at[name], rest = rest % size, rest // size
        to = {**at, **dest(at)}
        j = 0
        for name, size in zip(AXES, SIZES):
            j = j * size + to[name]
        pairs.append((i, j))
    return lax.ppermute(values, AXES, pairs)


def along(axis, by):
    def dest(at):
        if axis == "z":
            z = (at["zh"] * 2 + at["zl"] + by) % 4
            return {"zh": z // 2, "zl": z % 2}
        return {axis: (at[axis] + by) % 4}

    return dest


def by_core(first, second):
    return lambda at: (first if at["c"] == 0 else second)(at)


def swap(x, axis):
    return lax.ppermute(x, axis, [(0, 1), (1, 0)])


def pick(x, index, dim):
    return lax.dynamic_index_in_dim(x, index, dim, keepdims=False)


def place_kernel(idx, own, up, down, far, own2, up2, down2, far2, out, sems):
    c, a_at, b_at = idx[0], idx[1], idx[2]
    zh = idx[3]
    copies = []

    def put(pieces, a_first, b):
        for i in range(2):
            for j in range(2):
                a = a_first + i - 2 * i * (a_first % 2)
                z = zh + j - 2 * j * zh
                at_x = jnp.where(c == 0, a, b)
                at_y = jnp.where(c == 0, b, a)
                copies.append(
                    pltpu.make_async_copy(
                        pieces.at[i, j], out.at[z, at_x, at_y], sems.at[len(copies)]
                    )
                )

    for first, group in ((a_at, (own, up, down, far)), (3 - a_at, (own2, up2, down2, far2))):
        for pieces, back in zip(group, (0, 3, 1, 2)):
            put(pieces, first, (b_at + back) % 4)
    for copy in copies:
        copy.start()
    for copy in copies:
        copy.wait()


def nearest(at):
    z = 3 - (at["zh"] * 2 + at["zl"])
    return {"zh": z // 2, "zl": z % 2}


def place(idx, pieces, lanes):
    rows = pieces[0].shape[2]
    out = pl.pallas_call(
        place_kernel,
        out_shape=jax.ShapeDtypeStruct((2, 4, 4, rows, lanes), BF),
        in_specs=[pl.BlockSpec(memory_space=pltpu.SMEM)]
        + [pl.BlockSpec(memory_space=pltpu.HBM)] * 8,
        out_specs=pl.BlockSpec(memory_space=pltpu.VMEM),
        scratch_shapes=[pltpu.SemaphoreType.DMA((32,))],
        compiler_params=pltpu.CompilerParams(vmem_limit_bytes=24 << 20),
        cost_estimate=pl.CostEstimate(
            flops=0, transcendentals=0, bytes_accessed=128 * rows * lanes
        ),
        name="place",
    )(idx, *pieces)
    return out.reshape(32 * rows, lanes)


def flip_kernel(x, out):
    out[...] = x[...].T


def flip(x):
    rows, cols = x.shape
    step = 384
    return pl.pallas_call(
        flip_kernel,
        grid=(cols // step,),
        out_shape=jax.ShapeDtypeStruct((cols, rows), x.dtype),
        in_specs=[pl.BlockSpec((rows, step), lambda i: (0, i))],
        out_specs=pl.BlockSpec((step, rows), lambda i: (i, 0)),
        cost_estimate=pl.CostEstimate(flops=0, transcendentals=0, bytes_accessed=4 * rows * cols),
        name="flip",
    )(x)


def conv_kernel(feat, before, normed, kernels, out_kernel, out):
    b, n = before[...], normed[...]
    channels = n.shape[-1]
    middle = jnp.concatenate([b[:, 1:], n[:, :1]], axis=1)
    total = None
    for k, window in enumerate((b, middle, n)):
        part = jnp.dot(
            window.reshape(-1, channels), kernels[k], preferred_element_type=F32
        )
        total = part if total is None else total + part
    activation = feat[...].astype(F32).reshape(total.shape)
    stored = (activation + total / (1.0 + jnp.exp(-total))).astype(BF)
    latent = jnp.dot(stored, out_kernel[...], preferred_element_type=F32)
    out[...] = latent.astype(BF).reshape(out.shape)


def conv_clips(features, first, before, normed, kernels, out_kernel):
    clips, frames, pixels, channels = normed.shape
    step, lat = 8, out_kernel.shape[1]
    block = pl.BlockSpec((step, frames, pixels, channels), lambda i: (i, 0, 0, 0))
    return pl.pallas_call(
        conv_kernel,
        grid=(clips // step,),
        out_shape=jax.ShapeDtypeStruct((clips, frames, pixels, lat), BF),
        in_specs=[
            pl.BlockSpec(
                (step, frames, pixels, channels), lambda i: (i + first // step, 0, 0, 0)
            ),
            block,
            block,
            pl.BlockSpec(kernels.shape, lambda i: (0, 0, 0)),
            pl.BlockSpec(out_kernel.shape, lambda i: (0, 0)),
        ],
        out_specs=pl.BlockSpec((step, frames, pixels, lat), lambda i: (i, 0, 0, 0)),
        compiler_params=pltpu.CompilerParams(
            dimension_semantics=("arbitrary",), vmem_limit_bytes=32 << 20
        ),
        cost_estimate=pl.CostEstimate(
            flops=clips * frames * pixels * channels * channels * 6,
            transcendentals=0,
            bytes_accessed=4 << 20,
        ),
        name="conv",
    )(features, before, normed, kernels, out_kernel)


def unit_of(tok, embed):
    mixed = lax.dot_general(
        tok, embed, (((1,), (1,)), ((), ())), preferred_element_type=F32
    )
    centred = mixed - jnp.mean(mixed, axis=-1, keepdims=True)
    inv_std = lax.rsqrt(jnp.mean(centred * centred, axis=-1, keepdims=True) + 1e-06)
    return centred * inv_std, inv_std


def forward_kernel(idx, tok, embed, scale, shift, out_all, out_kept, out_given):
    c = idx[0]
    unit, _ = unit_of(tok[...], embed[...])
    out_all[...] = (unit * (1.0 + scale[...]) + shift[...]).astype(BF)
    quarter = out_all.shape[1] // 4
    for zl in range(2):
        here = pl.ds(zl * quarter, quarter)
        at = pl.multiple_of((2 * zl + c) * quarter, 128)
        out_kept[:, here] = out_all[:, pl.ds(at, quarter)]
        at = pl.multiple_of((2 * zl + 1 - c) * quarter, 128)
        out_given[:, here] = out_all[:, pl.ds(at, quarter)]


def backward_kernel(
    idx, tok_t, tok, embed, scaling, cot_t, w_kept, w_got, out_e, grad_ref, mixed_ref, grad_bf, acc
):
    c, step = idx[0], pl.program_id(0)
    block, half = w_kept.shape
    width, lanes = grad_ref.shape
    group = 32

    def against(at, weight):
        at = pl.multiple_of(at * half, 128)
        return jnp.dot(weight[...], cot_t[pl.ds(at, half), :], preferred_element_type=F32)

    rows = pl.ds(pl.multiple_of(step * block, block), block)
    factor = jnp.concatenate([scaling[...]] * (lanes // scaling.shape[1]), axis=1)
    grad_ref[rows, :] = (against(c, w_kept) + against(1 - c, w_got)) * factor
    mixed_ref[rows, :] = jnp.dot(
        embed[...], tok_t[...], preferred_element_type=F32
    )

    @pl.when(step == 0)
    def _():
        acc[...] = jnp.zeros(acc.shape, F32)

    origin = mixed_ref[0:1, :]

    def load(first, i):
        here = pl.ds(pl.multiple_of(first + i * group, group), group)
        return here, mixed_ref[here, :] - origin, grad_ref[here, :]

    def fold(v):
        return jnp.sum(v.reshape(group // 8, 8, lanes), axis=0)

    def sums(i, carry):
        _, shifted, grad = load(step * block, i)
        for k, v in enumerate((shifted, shifted * shifted, grad, grad * shifted)):
            acc[k] += fold(v)
        return carry

    lax.fori_loop(0, block // group, sums, 0)

    @pl.when(step == pl.num_programs(0) - 1)
    def _():
        mean, square, mean_g, product = (
            jnp.sum(acc[k], axis=0, keepdims=True) * (1.0 / width) for k in range(4)
        )
        inv_std = lax.rsqrt(jnp.maximum(square - mean * mean, 0.0) + 1e-06)
        slope = (product - mean * mean_g) * inv_std * inv_std

        def finish(i, carry):
            here, shifted, grad = load(0, i)
            grad_bf[here, :] = (inv_std * (grad - mean_g - (shifted - mean) * slope)).astype(BF)
            return carry

        lax.fori_loop(0, width // group, finish, 0)
        out_e[...] = jnp.dot(grad_bf[...], tok[...], preferred_element_type=F32)


def backward_call(core, tok_t, tok, embed, scaling, cot_t, w_kept, w_got):
    width, tokens, block = embed.shape[0], tok.shape[0], 512

    def stays(a):
        return pl.BlockSpec(a.shape, lambda i, _: (0, 0))

    def by_rows(a):
        return pl.BlockSpec((block, a.shape[1]), lambda i, _: (i, 0))

    return pl.pallas_call(
        backward_kernel,
        grid_spec=pltpu.PrefetchScalarGridSpec(
            num_scalar_prefetch=1,
            grid=(width // block,),
            in_specs=[
                stays(tok_t),
                stays(tok),
                by_rows(embed),
                by_rows(scaling),
                stays(cot_t),
                by_rows(w_kept),
                by_rows(w_got),
            ],
            out_specs=pl.BlockSpec((width, tok.shape[1]), lambda i, _: (0, 0)),
            scratch_shapes=[
                pltpu.VMEM((width, tokens), F32),
                pltpu.VMEM((width, tokens), F32),
                pltpu.VMEM((width, tokens), BF),
                pltpu.VMEM((4, 8, tokens), F32),
            ],
        ),
        out_shape=jax.ShapeDtypeStruct((width, tok.shape[1]), F32),
        compiler_params=pltpu.CompilerParams(
            dimension_semantics=("arbitrary",), vmem_limit_bytes=40 << 20
        ),
        cost_estimate=pl.CostEstimate(
            flops=2 * tokens * width * cot_t.shape[0],
            transcendentals=0,
            bytes_accessed=16 << 20,
        ),
        name="backward",
    )(core, tok_t, tok, embed, scaling, cot_t, w_kept, w_got)


def values_kernel(idx, mod, weight, *rest):
    rest[-1][...] = jnp.dot(mod[...], weight[...], preferred_element_type=F32).astype(BF)


def values_call(side, mod, weight, before=None):
    tokens, width = mod.shape
    half, step = weight.shape[1], 256
    steps = half // step
    rest = [] if before is None else [before]
    return pl.pallas_call(
        values_kernel,
        grid_spec=pltpu.PrefetchScalarGridSpec(
            num_scalar_prefetch=1,
            grid=(steps,),
            in_specs=[
                pl.BlockSpec((tokens, width), lambda i, _: (0, 0)),
                pl.BlockSpec((width, step), lambda i, _: (0, i)),
            ]
            + [pl.BlockSpec(memory_space=pl.ANY)] * len(rest),
            out_specs=pl.BlockSpec((tokens, step), lambda i, idx: (0, idx[0] * steps + i)),
        ),
        out_shape=jax.ShapeDtypeStruct((tokens, 2 * half), BF),
        input_output_aliases={} if before is None else {3: 0},
        compiler_params=pltpu.CompilerParams(
            dimension_semantics=("arbitrary",), vmem_limit_bytes=32 << 20
        ),
        cost_estimate=pl.CostEstimate(
            flops=2 * tokens * width * half, transcendentals=0, bytes_accessed=7 << 20
        ),
        name="values",
    )(side, mod, weight, *rest)


def rows_call(kernel, idx, blocked, whole, outs, flops=0):
    tokens, step = blocked[0].shape[0], 256

    def by_rows(a):
        return pl.BlockSpec((step, a.shape[1]), lambda i, _: (i, 0))

    def stays(a):
        return pl.BlockSpec(a.shape, lambda i, _: (0, 0))

    return pl.pallas_call(
        kernel,
        grid_spec=pltpu.PrefetchScalarGridSpec(
            num_scalar_prefetch=1,
            grid=(tokens // step,),
            in_specs=[stays(a) if a_whole else by_rows(a) for a, a_whole in zip(blocked, whole)],
            out_specs=[by_rows(o) if o.shape[0] == tokens else stays(o) for o in outs],
        ),
        out_shape=outs,
        compiler_params=pltpu.CompilerParams(
            dimension_semantics=("arbitrary",), vmem_limit_bytes=48 << 20
        ),
        cost_estimate=pl.CostEstimate(flops=flops, transcendentals=0, bytes_accessed=16 << 20),
    )(idx, *blocked)


def exchange(latent, embed_weight, assign):
    clips, rows = latent.shape[0], embed_weight.shape[0]
    ordered = jnp.take(latent, assign, axis=0).reshape(clips, -1, 128)
    packed = jnp.concatenate([embed_weight[: rows // 2], embed_weight[rows // 2 :]], axis=1)
    packed = jnp.broadcast_to(packed, (clips,) + packed.shape)
    both = jnp.concatenate([packed, ordered], axis=1)
    both = lax.all_to_all(both, ("zh", "x", "y"), split_axis=0, concat_axis=0, tiled=True)
    embed = both[:, : rows // 2]
    embed = jnp.concatenate([embed[..., :64], embed[..., 64:]], axis=1).reshape(-1, 64)
    frames = latent.shape[1]
    tokens = both[:, rows // 2 :].reshape(clips, frames, -1, 64)
    return jnp.swapaxes(tokens, 0, 1).reshape(-1, 64), embed


def ring_reduce(part, cut, forward, back, beside=None):
    def halves(p):
        return p[:cut], p[cut:]

    far_a, far_b = halves(part(2))
    up_a, up_b = halves(part(1))
    down_a, down_b = halves(part(3))
    own_a, own_b = halves(part(0))
    send_f = jnp.concatenate([far_a, up_b], axis=0)
    send_b = jnp.concatenate([far_b, down_a], axis=0)
    got_f = hop(send_f, forward)
    got_b = hop(send_b, back)
    tied = lax.optimization_barrier
    one = None
    if beside is not None:
        one = beside((send_f, send_b))
        got_f, got_b, one = tied((got_f, got_b, one))
    from_a, from_b = got_f[:cut], got_b[:cut]
    sum_a = (up_a.astype(F32) + from_a.astype(F32)).astype(BF)
    sum_b = (down_b.astype(F32) + from_b.astype(F32)).astype(BF)
    last_a = hop(sum_a, forward)
    last_b = hop(sum_b, back)
    last_a, last_b, got_f, got_b = tied((last_a, last_b, got_f, got_b))
    near_b, near_a = got_f[cut:], got_b[cut:]
    a = own_a.astype(F32) + near_a.astype(F32) + last_a.astype(F32)
    b = own_b.astype(F32) + near_b.astype(F32) + last_b.astype(F32)
    return jnp.concatenate([a, b], axis=0), one


def direct_reduce(part, dest):
    total = part(0).astype(F32)
    for d in (1, 3, 2):
        got = hop(part(d), dest(d))
        total = total + got.astype(F32)
    return total


def channel_norm(activation, gain_row):
    scaling = lax.rsqrt(jnp.mean(activation * activation, axis=-1, keepdims=True) + 1e-06)
    return activation * scaling * gain_row


def norm_clips(enc_features, enc_gain, clip_start):
    frame_count = enc_features.shape[1]
    enc_index = lax.axis_index("zl") * 2 + lax.axis_index("c")
    frame_ids = enc_index * frame_count + jnp.arange(frame_count, dtype=jnp.int32)
    live_mask = (frame_ids[None, :] >= clip_start[:, None]).astype(F32)[:, :, None, None]
    normed = live_mask * channel_norm(enc_features.astype(F32), enc_gain[0])
    return normed.astype(BF), live_mask


def as_patches(latent, live_mask):
    clips, frames, pixels, lat = latent.shape
    latent = latent * live_mask.astype(BF)
    return latent.reshape(clips, frames, pixels // 4, 4 * lat)


def local(
    enc_features,
    enc_gain,
    enc_kernel,
    out_kernel,
    clip_start,
    assign,
    embed_weight,
    mod_shift,
    mod_scale,
    value_weight,
    value_cotangent,
):
    pos = {name: lax.axis_index(name) for name in AXES}
    c = pos["c"]
    cols = value_cotangent.shape[-1]
    half = cols // 2
    cot_rows = value_cotangent.reshape(-1, cols)
    tokens = cot_rows.shape[0]
    tied = lax.optimization_barrier
    zh, x, y = pos["zh"], pos["x"], pos["y"]
    rows = value_weight.shape[0]
    own = lax.dynamic_slice_in_dim(value_weight, c * half, half, axis=1)
    a_at = jnp.where(c == 0, x, y)
    b_at = jnp.where(c == 0, y, x)
    got_z = hop(own, nearest)
    bounds = (0, 16, 32)
    kernels = pltpu.with_memory_space_constraint(enc_kernel[0], pltpu.HBM)

    def group(k, features):
        part = slice(*bounds[k : k + 2])
        normed, live_mask = norm_clips(features[part], enc_gain, clip_start[part])
        before = lax.ppermute(normed, ("zl", "c"), [(0, 1), (1, 2), (2, 3)])
        return normed, before, live_mask

    def latents(k, normed, before, live_mask):
        latent = conv_clips(
            enc_features, bounds[k], before, normed, kernels, out_kernel
        )
        return as_patches(latent, live_mask)

    group_a = group(0, enc_features)
    got_z, _ = tied((got_z, group_a[0]))
    pair = jnp.stack([own, got_z])
    one = hop(pair, by_core(lambda at: {"x": at["x"] ^ 1}, lambda at: {"y": at["y"] ^ 1}))
    features, _ = tied((enc_features, got_z))
    group_b = group(1, features)
    one, _ = tied((one, group_b[0]))
    other_cot = swap(cot_rows, "c")
    two = jnp.stack([pair, one])
    four = hop(two, by_core(lambda at: {"x": 3 - at["x"]}, lambda at: {"y": 3 - at["y"]}))
    ahead = by_core(along("y", 1), along("x", 1))
    behind = by_core(along("y", 3), along("x", 3))
    up = hop(two, ahead)
    down = hop(two, behind)

    latent_a = latents(0, *group_a)
    up2 = hop(four, ahead)
    down2 = hop(four, behind)
    far = hop(up, ahead)
    latent_b = latents(1, *group_b)
    token_rows, embed_full = exchange(jnp.concatenate([latent_a, latent_b]), embed_weight, assign)
    late_cot, late_scale, _ = tied((cot_rows, mod_scale, latent_b))
    cot_t = flip(late_cot)
    scaling = jnp.broadcast_to((1.0 + late_scale).reshape(-1, 1), (mod_scale.shape[1], 128))
    far2 = hop(down2, behind)
    idx = jnp.stack([c, a_at, b_at, zh]).astype(jnp.int32)
    pieces = (two, up, down, far, four, up2, down2, far2)
    width = embed_full.shape[0]
    quarter = width // 4
    core = jnp.reshape(c, (1,)).astype(jnp.int32)

    modulated, kept, given = rows_call(
        forward_kernel,
        core,
        (token_rows, embed_full, mod_scale, mod_shift),
        (False, True, True, True),
        [
            jax.ShapeDtypeStruct((tokens, width), BF),
            jax.ShapeDtypeStruct((tokens, width // 2), BF),
            jax.ShapeDtypeStruct((tokens, width // 2), BF),
        ],
        flops=2 * tokens * width * 512,
    )
    got = swap(given, "c")
    weight_kept = place(idx, pieces, half)
    weight_got = swap(weight_kept, "c")
    mod_rows = jnp.concatenate([kept, got], axis=0)
    cot_both = jnp.concatenate([cot_rows, other_cot], axis=0)
    grad_w = lax.dot_general(
        mod_rows, cot_both, (((0,), (0,)), ((), ())), preferred_element_type=F32
    ).astype(BF)
    blocks_w = grad_w.reshape(4, 4, 96, cols)

    def x_at(d):
        return (pos["x"] + d) % 4

    def z_at(d):
        z = (pos["zh"] * 2 + pos["zl"] + d) % 4
        return (z % 2) * 2 + z // 2

    def cut(blocks, d):
        return jnp.where(c == 0, pick(blocks, x_at(d), 1), pick(blocks, z_at(d), 0))

    projected = values_call(core, modulated, weight_kept)

    def embed_gradient(after):
        tok, _ = tied((token_rows, after))
        grad_e = backward_call(
            core, tok.T, tok, embed_full, scaling, cot_t, weight_kept, weight_got
        )
        grad_e = grad_e.reshape(2, 2, quarter, -1)
        given = swap(pick(grad_e, 1 - c, 1).astype(BF), "c")
        return grad_e, given

    projected = values_call(1 - core, modulated, weight_got, projected)

    forward = by_core(along("x", 1), along("z", 1))
    back = by_core(along("x", 3), along("z", 3))
    chunk, (grad_e, given_e) = ring_reduce(
        lambda d: cut(blocks_w, d), 2, forward, back, embed_gradient
    )
    grad_e = (pick(grad_e, c, 1) + given_e.astype(F32)).astype(BF).reshape(4, 4, 96, -1)
    chunk_e = direct_reduce(
        lambda d: cut(grad_e, d), lambda d: by_core(along("x", d), along("z", d))
    )
    chunk = jnp.concatenate([chunk.astype(BF), chunk_e.astype(BF)], axis=-1)

    def second(d):
        return pick(chunk, jnp.where(c == 0, z_at(d), x_at(d)), 0)

    rows = direct_reduce(second, lambda d: by_core(along("z", d), along("x", d)))
    rows = rows.reshape(4, 24, -1)
    summed = direct_reduce(lambda d: pick(rows, (pos["y"] + d) % 4, 0), lambda d: along("y", d))
    grad_value = summed[:, :cols]
    grad_embed = summed[:, cols:]

    return (projected.reshape(value_cotangent.shape), grad_value, grad_embed)


def solution(mesh):
    sub = Mesh(mesh.devices.reshape(SIZES), AXES)
    enc, fsdp = ("zl", "c"), ("zh", "x", "y")
    in_specs = (
        P(None, enc, fsdp, None),
        P(),
        P(),
        P(),
        P(),
        P(),
        P(fsdp, None),
        P(fsdp, None),
        P(fsdp, None),
        P(fsdp, None),
        P(fsdp, enc, None, None),
    )
    out_specs = (P(fsdp, enc, None, None), P(enc + fsdp, None), P(enc + fsdp, None))
    return jax.shard_map(local, mesh=sub, in_specs=in_specs, out_specs=out_specs, check_vma=False)
```

```python
import jax
import jax.numpy as jnp
from jax import lax
from jax.experimental import pallas as pl
from jax.experimental.pallas import tpu as pltpu
from jax.sharding import Mesh
from jax.sharding import PartitionSpec as P


BF = jnp.bfloat16
F32 = jnp.float32
AXES = ("zl", "c", "zh", "x", "y")
SIZES = (2, 2, 2, 4, 4)


def hop(values, dest):
    pairs = []
    for i in range(128):
        at, rest = {}, i
        for name, size in zip(reversed(AXES), reversed(SIZES)):
            at[name], rest = rest % size, rest // size
        to = {**at, **dest(at)}
        j = 0
        for name, size in zip(AXES, SIZES):
            j = j * size + to[name]
        pairs.append((i, j))
    return lax.ppermute(values, AXES, pairs)


def along(axis, by):
    def dest(at):
        if axis == "z":
            z = (at["zh"] * 2 + at["zl"] + by) % 4
            return {"zh": z // 2, "zl": z % 2}
        return {axis: (at[axis] + by) % 4}

    return dest


def by_core(first, second):
    return lambda at: (first if at["c"] == 0 else second)(at)


def swap(x, axis):
    return lax.ppermute(x, axis, [(0, 1), (1, 0)])


def pick(x, index, dim):
    return lax.dynamic_index_in_dim(x, index, dim, keepdims=False)


def place_kernel(idx, own, up, down, far, own2, up2, down2, far2, out, sems):
    c, a_at, b_at = idx[0], idx[1], idx[2]
    zh = idx[3]
    copies = []

    def put(pieces, a_first, b):
        for i in range(2):
            for j in range(2):
                a = a_first + i - 2 * i * (a_first % 2)
                z = zh + j - 2 * j * zh
                at_x = jnp.where(c == 0, a, b)
                at_y = jnp.where(c == 0, b, a)
                copies.append(
                    pltpu.make_async_copy(
                        pieces.at[i, j], out.at[z, at_x, at_y], sems.at[len(copies)]
                    )
                )

    for first, group in ((a_at, (own, up, down, far)), (3 - a_at, (own2, up2, down2, far2))):
        for pieces, back in zip(group, (0, 3, 1, 2)):
            put(pieces, first, (b_at + back) % 4)
    for copy in copies:
        copy.start()
    for copy in copies:
        copy.wait()


def nearest(at):
    z = 3 - (at["zh"] * 2 + at["zl"])
    return {"zh": z // 2, "zl": z % 2}


def place(idx, pieces, lanes):
    rows = pieces[0].shape[2]
    out = pl.pallas_call(
        place_kernel,
        out_shape=jax.ShapeDtypeStruct((2, 4, 4, rows, lanes), BF),
        in_specs=[pl.BlockSpec(memory_space=pltpu.SMEM)]
        + [pl.BlockSpec(memory_space=pltpu.HBM)] * 8,
        out_specs=pl.BlockSpec(memory_space=pltpu.VMEM),
        scratch_shapes=[pltpu.SemaphoreType.DMA((32,))],
        compiler_params=pltpu.CompilerParams(vmem_limit_bytes=24 << 20),
        cost_estimate=pl.CostEstimate(
            flops=0, transcendentals=0, bytes_accessed=128 * rows * lanes
        ),
        name="place",
    )(idx, *pieces)
    return out.reshape(32 * rows, lanes)


def flip_kernel(x, out):
    out[...] = x[...].T


def flip(x):
    rows, cols = x.shape
    step = 384
    return pl.pallas_call(
        flip_kernel,
        grid=(cols // step,),
        out_shape=jax.ShapeDtypeStruct((cols, rows), x.dtype),
        in_specs=[pl.BlockSpec((rows, step), lambda i: (0, i))],
        out_specs=pl.BlockSpec((step, rows), lambda i: (i, 0)),
        cost_estimate=pl.CostEstimate(flops=0, transcendentals=0, bytes_accessed=4 * rows * cols),
        name="flip",
    )(x)


def conv_kernel(feat, before, normed, kernels, out_kernel, out):
    b, n = before[...], normed[...]
    channels = n.shape[-1]
    middle = jnp.concatenate([b[:, 1:], n[:, :1]], axis=1)
    total = None
    for k, window in enumerate((b, middle, n)):
        part = jnp.dot(
            window.reshape(-1, channels), kernels[k], preferred_element_type=F32
        )
        total = part if total is None else total + part
    activation = feat[...].astype(F32).reshape(total.shape)
    stored = (activation + total / (1.0 + jnp.exp(-total))).astype(BF)
    latent = jnp.dot(stored, out_kernel[...], preferred_element_type=F32)
    out[...] = latent.astype(BF).reshape(out.shape)


def conv_clips(features, first, before, normed, kernels, out_kernel):
    clips, frames, pixels, channels = normed.shape
    step, lat = 8, out_kernel.shape[1]
    block = pl.BlockSpec((step, frames, pixels, channels), lambda i: (i, 0, 0, 0))
    return pl.pallas_call(
        conv_kernel,
        grid=(clips // step,),
        out_shape=jax.ShapeDtypeStruct((clips, frames, pixels, lat), BF),
        in_specs=[
            pl.BlockSpec(
                (step, frames, pixels, channels), lambda i: (i + first // step, 0, 0, 0)
            ),
            block,
            block,
            pl.BlockSpec(kernels.shape, lambda i: (0, 0, 0)),
            pl.BlockSpec(out_kernel.shape, lambda i: (0, 0)),
        ],
        out_specs=pl.BlockSpec((step, frames, pixels, lat), lambda i: (i, 0, 0, 0)),
        compiler_params=pltpu.CompilerParams(
            dimension_semantics=("arbitrary",), vmem_limit_bytes=32 << 20
        ),
        cost_estimate=pl.CostEstimate(
            flops=clips * frames * pixels * channels * channels * 6,
            transcendentals=0,
            bytes_accessed=4 << 20,
        ),
        name="conv",
    )(features, before, normed, kernels, out_kernel)


def unit_of(tok, embed):
    mixed = lax.dot_general(
        tok, embed, (((1,), (1,)), ((), ())), preferred_element_type=F32
    )
    centred = mixed - jnp.mean(mixed, axis=-1, keepdims=True)
    inv_std = lax.rsqrt(jnp.mean(centred * centred, axis=-1, keepdims=True) + 1e-06)
    return centred * inv_std, inv_std


def forward_kernel(idx, tok, embed, scale, shift, out_all, out_kept, out_given):
    c = idx[0]
    unit, _ = unit_of(tok[...], embed[...])
    out_all[...] = (unit * (1.0 + scale[...]) + shift[...]).astype(BF)
    quarter = out_all.shape[1] // 4
    for zl in range(2):
        here = pl.ds(zl * quarter, quarter)
        at = pl.multiple_of((2 * zl + c) * quarter, 128)
        out_kept[:, here] = out_all[:, pl.ds(at, quarter)]
        at = pl.multiple_of((2 * zl + 1 - c) * quarter, 128)
        out_given[:, here] = out_all[:, pl.ds(at, quarter)]


def backward_kernel(
    idx, tok_t, tok, embed, scaling, cot_t, w_kept, w_got, out_e, grad_ref, mixed_ref, grad_bf, acc
):
    c, step = idx[0], pl.program_id(0)
    block, half = w_kept.shape
    width, lanes = grad_ref.shape
    group = 32

    def against(at, weight):
        at = pl.multiple_of(at * half, 128)
        return jnp.dot(weight[...], cot_t[pl.ds(at, half), :], preferred_element_type=F32)

    rows = pl.ds(pl.multiple_of(step * block, block), block)
    factor = jnp.concatenate([scaling[...]] * (lanes // scaling.shape[1]), axis=1)
    grad_ref[rows, :] = (against(c, w_kept) + against(1 - c, w_got)) * factor
    mixed_ref[rows, :] = jnp.dot(
        embed[...], tok_t[...], preferred_element_type=F32
    )

    @pl.when(step == 0)
    def _():
        acc[...] = jnp.zeros(acc.shape, F32)

    origin = mixed_ref[0:1, :]

    def load(first, i):
        here = pl.ds(pl.multiple_of(first + i * group, group), group)
        return here, mixed_ref[here, :] - origin, grad_ref[here, :]

    def fold(v):
        return jnp.sum(v.reshape(group // 8, 8, lanes), axis=0)

    def sums(i, carry):
        _, shifted, grad = load(step * block, i)
        for k, v in enumerate((shifted, shifted * shifted, grad, grad * shifted)):
            acc[k] += fold(v)
        return carry

    lax.fori_loop(0, block // group, sums, 0)

    @pl.when(step == pl.num_programs(0) - 1)
    def _():
        mean, square, mean_g, product = (
            jnp.sum(acc[k], axis=0, keepdims=True) * (1.0 / width) for k in range(4)
        )
        inv_std = lax.rsqrt(jnp.maximum(square - mean * mean, 0.0) + 1e-06)
        slope = (product - mean * mean_g) * inv_std * inv_std

        def finish(i, carry):
            here, shifted, grad = load(0, i)
            grad_bf[here, :] = (inv_std * (grad - mean_g - (shifted - mean) * slope)).astype(BF)
            return carry

        lax.fori_loop(0, width // group, finish, 0)
        out_e[...] = jnp.dot(grad_bf[...], tok[...], preferred_element_type=F32)


def backward_call(core, tok_t, tok, embed, scaling, cot_t, w_kept, w_got):
    width, tokens, block = embed.shape[0], tok.shape[0], 512

    def stays(a):
        return pl.BlockSpec(a.shape, lambda i, _: (0, 0))

    def by_rows(a):
        return pl.BlockSpec((block, a.shape[1]), lambda i, _: (i, 0))

    return pl.pallas_call(
        backward_kernel,
        grid_spec=pltpu.PrefetchScalarGridSpec(
            num_scalar_prefetch=1,
            grid=(width // block,),
            in_specs=[
                stays(tok_t),
                stays(tok),
                by_rows(embed),
                by_rows(scaling),
                stays(cot_t),
                by_rows(w_kept),
                by_rows(w_got),
            ],
            out_specs=pl.BlockSpec((width, tok.shape[1]), lambda i, _: (0, 0)),
            scratch_shapes=[
                pltpu.VMEM((width, tokens), F32),
                pltpu.VMEM((width, tokens), F32),
                pltpu.VMEM((width, tokens), BF),
                pltpu.VMEM((4, 8, tokens), F32),
            ],
        ),
        out_shape=jax.ShapeDtypeStruct((width, tok.shape[1]), F32),
        compiler_params=pltpu.CompilerParams(
            dimension_semantics=("arbitrary",), vmem_limit_bytes=40 << 20
        ),
        cost_estimate=pl.CostEstimate(
            flops=2 * tokens * width * cot_t.shape[0],
            transcendentals=0,
            bytes_accessed=16 << 20,
        ),
        name="backward",
    )(core, tok_t, tok, embed, scaling, cot_t, w_kept, w_got)


def values_kernel(idx, mod, weight, *rest):
    rest[-1][...] = jnp.dot(mod[...], weight[...], preferred_element_type=F32).astype(BF)


def values_call(side, mod, weight, before=None):
    tokens, width = mod.shape
    half, step = weight.shape[1], 256
    steps = half // step
    rest = [] if before is None else [before]
    return pl.pallas_call(
        values_kernel,
        grid_spec=pltpu.PrefetchScalarGridSpec(
            num_scalar_prefetch=1,
            grid=(steps,),
            in_specs=[
                pl.BlockSpec((tokens, width), lambda i, _: (0, 0)),
                pl.BlockSpec((width, step), lambda i, _: (0, i)),
            ]
            + [pl.BlockSpec(memory_space=pl.ANY)] * len(rest),
            out_specs=pl.BlockSpec((tokens, step), lambda i, idx: (0, idx[0] * steps + i)),
        ),
        out_shape=jax.ShapeDtypeStruct((tokens, 2 * half), BF),
        input_output_aliases={} if before is None else {3: 0},
        compiler_params=pltpu.CompilerParams(
            dimension_semantics=("arbitrary",), vmem_limit_bytes=32 << 20
        ),
        cost_estimate=pl.CostEstimate(
            flops=2 * tokens * width * half, transcendentals=0, bytes_accessed=7 << 20
        ),
        name="values",
    )(side, mod, weight, *rest)


def rows_call(kernel, idx, blocked, whole, outs, flops=0):
    tokens, step = blocked[0].shape[0], 256

    def by_rows(a):
        return pl.BlockSpec((step, a.shape[1]), lambda i, _: (i, 0))

    def stays(a):
        return pl.BlockSpec(a.shape, lambda i, _: (0, 0))

    return pl.pallas_call(
        kernel,
        grid_spec=pltpu.PrefetchScalarGridSpec(
            num_scalar_prefetch=1,
            grid=(tokens // step,),
            in_specs=[stays(a) if a_whole else by_rows(a) for a, a_whole in zip(blocked, whole)],
            out_specs=[by_rows(o) if o.shape[0] == tokens else stays(o) for o in outs],
        ),
        out_shape=outs,
        compiler_params=pltpu.CompilerParams(
            dimension_semantics=("arbitrary",), vmem_limit_bytes=48 << 20
        ),
        cost_estimate=pl.CostEstimate(flops=flops, transcendentals=0, bytes_accessed=16 << 20),
    )(idx, *blocked)


def exchange(latent, embed_weight, assign):
    clips, rows = latent.shape[0], embed_weight.shape[0]
    ordered = jnp.take(latent, assign, axis=0).reshape(clips, -1, 128)
    packed = jnp.concatenate([embed_weight[: rows // 2], embed_weight[rows // 2 :]], axis=1)
    packed = jnp.broadcast_to(packed, (clips,) + packed.shape)
    both = jnp.concatenate([packed, ordered], axis=1)
    both = lax.all_to_all(both, ("zh", "x", "y"), split_axis=0, concat_axis=0, tiled=True)
    embed = both[:, : rows // 2]
    embed = jnp.concatenate([embed[..., :64], embed[..., 64:]], axis=1).reshape(-1, 64)
    frames = latent.shape[1]
    tokens = both[:, rows // 2 :].reshape(clips, frames, -1, 64)
    return jnp.swapaxes(tokens, 0, 1).reshape(-1, 64), embed


def ring_reduce(part, cut, forward, back, beside=None):
    def halves(p):
        return p[:cut], p[cut:]

    far_a, far_b = halves(part(2))
    up_a, up_b = halves(part(1))
    down_a, down_b = halves(part(3))
    own_a, own_b = halves(part(0))
    send_f = jnp.concatenate([far_a, up_b], axis=0)
    send_b = jnp.concatenate([far_b, down_a], axis=0)
    got_f = hop(send_f, forward)
    got_b = hop(send_b, back)
    tied = lax.optimization_barrier
    one = None
    if beside is not None:
        one = beside((send_f, send_b))
        got_f, got_b, one = tied((got_f, got_b, one))
    from_a, from_b = got_f[:cut], got_b[:cut]
    sum_a = (up_a.astype(F32) + from_a.astype(F32)).astype(BF)
    sum_b = (down_b.astype(F32) + from_b.astype(F32)).astype(BF)
    last_a = hop(sum_a, forward)
    last_b = hop(sum_b, back)
    last_a, last_b, got_f, got_b = tied((last_a, last_b, got_f, got_b))
    near_b, near_a = got_f[cut:], got_b[cut:]
    a = own_a.astype(F32) + near_a.astype(F32) + last_a.astype(F32)
    b = own_b.astype(F32) + near_b.astype(F32) + last_b.astype(F32)
    return jnp.concatenate([a, b], axis=0), one


def direct_pieces(part, dest):
    pieces = [part(0)]
    for d in (1, 3, 2):
        pieces.append(hop(part(d), dest(d)))
    return pieces


def add_up(pieces):
    total = pieces[0].astype(F32)
    for piece in pieces[1:]:
        total = total + piece.astype(F32)
    return total


def channel_norm(activation, gain_row):
    scaling = lax.rsqrt(jnp.mean(activation * activation, axis=-1, keepdims=True) + 1e-06)
    return activation * scaling * gain_row


def norm_clips(enc_features, enc_gain, clip_start):
    frame_count = enc_features.shape[1]
    enc_index = lax.axis_index("zl") * 2 + lax.axis_index("c")
    frame_ids = enc_index * frame_count + jnp.arange(frame_count, dtype=jnp.int32)
    live_mask = (frame_ids[None, :] >= clip_start[:, None]).astype(F32)[:, :, None, None]
    normed = live_mask * channel_norm(enc_features.astype(F32), enc_gain[0])
    return normed.astype(BF), live_mask


def as_patches(latent, live_mask):
    clips, frames, pixels, lat = latent.shape
    latent = latent * live_mask.astype(BF)
    return latent.reshape(clips, frames, pixels // 4, 4 * lat)


def local(
    enc_features,
    enc_gain,
    enc_kernel,
    out_kernel,
    clip_start,
    assign,
    embed_weight,
    mod_shift,
    mod_scale,
    value_weight,
    value_cotangent,
):
    pos = {name: lax.axis_index(name) for name in AXES}
    c = pos["c"]
    cols = value_cotangent.shape[-1]
    half = cols // 2
    cot_rows = value_cotangent.reshape(-1, cols)
    tokens = cot_rows.shape[0]
    tied = lax.optimization_barrier
    zh, x, y = pos["zh"], pos["x"], pos["y"]
    rows = value_weight.shape[0]
    own = lax.dynamic_slice_in_dim(value_weight, c * half, half, axis=1)
    a_at = jnp.where(c == 0, x, y)
    b_at = jnp.where(c == 0, y, x)
    got_z = hop(own, nearest)
    bounds = (0, 16, 32)
    kernels = pltpu.with_memory_space_constraint(enc_kernel[0], pltpu.HBM)

    def group(k, features):
        part = slice(*bounds[k : k + 2])
        normed, live_mask = norm_clips(features[part], enc_gain, clip_start[part])
        before = lax.ppermute(normed, ("zl", "c"), [(0, 1), (1, 2), (2, 3)])
        return normed, before, live_mask

    def latents(k, normed, before, live_mask):
        latent = conv_clips(
            enc_features, bounds[k], before, normed, kernels, out_kernel
        )
        return as_patches(latent, live_mask)

    group_a = group(0, enc_features)
    got_z, _ = tied((got_z, group_a[0]))
    pair = jnp.stack([own, got_z])
    one = hop(pair, by_core(lambda at: {"x": at["x"] ^ 1}, lambda at: {"y": at["y"] ^ 1}))
    features, _ = tied((enc_features, got_z))
    group_b = group(1, features)
    one, _ = tied((one, group_b[0]))
    other_cot = swap(cot_rows, "c")
    two = jnp.stack([pair, one])
    four = hop(two, by_core(lambda at: {"x": 3 - at["x"]}, lambda at: {"y": 3 - at["y"]}))
    ahead = by_core(along("y", 1), along("x", 1))
    behind = by_core(along("y", 3), along("x", 3))
    up = hop(two, ahead)
    down = hop(two, behind)

    latent_a = latents(0, *group_a)
    up2 = hop(four, ahead)
    down2 = hop(four, behind)
    far = hop(up, ahead)
    latent_b = latents(1, *group_b)
    token_rows, embed_full = exchange(jnp.concatenate([latent_a, latent_b]), embed_weight, assign)
    late_cot, late_scale, _ = tied((cot_rows, mod_scale, latent_b))
    cot_t = flip(late_cot)
    scaling = jnp.broadcast_to((1.0 + late_scale).reshape(-1, 1), (mod_scale.shape[1], 128))
    far2 = hop(down2, behind)
    idx = jnp.stack([c, a_at, b_at, zh]).astype(jnp.int32)
    pieces = (two, up, down, far, four, up2, down2, far2)
    width = embed_full.shape[0]
    quarter = width // 4
    core = jnp.reshape(c, (1,)).astype(jnp.int32)

    modulated, kept, given = rows_call(
        forward_kernel,
        core,
        (token_rows, embed_full, mod_scale, mod_shift),
        (False, True, True, True),
        [
            jax.ShapeDtypeStruct((tokens, width), BF),
            jax.ShapeDtypeStruct((tokens, width // 2), BF),
            jax.ShapeDtypeStruct((tokens, width // 2), BF),
        ],
        flops=2 * tokens * width * 512,
    )
    got = swap(given, "c")
    weight_kept = place(idx, pieces, half)
    weight_got = swap(weight_kept, "c")
    mod_rows = jnp.concatenate([kept, got], axis=0)
    cot_both = jnp.concatenate([cot_rows, other_cot], axis=0)
    grad_w = lax.dot_general(
        mod_rows, cot_both, (((0,), (0,)), ((), ())), preferred_element_type=F32
    ).astype(BF)
    blocks_w = grad_w.reshape(4, 4, 96, cols)

    def x_at(d):
        return (pos["x"] + d) % 4

    def z_at(d):
        z = (pos["zh"] * 2 + pos["zl"] + d) % 4
        return (z % 2) * 2 + z // 2

    def cut(blocks, d):
        return jnp.where(c == 0, pick(blocks, x_at(d), 1), pick(blocks, z_at(d), 0))

    projected = values_call(core, modulated, weight_kept)

    def embed_gradient(after):
        tok, _ = tied((token_rows, after))
        grad_e = backward_call(
            core, tok.T, tok, embed_full, scaling, cot_t, weight_kept, weight_got
        )
        grad_e = grad_e.reshape(2, 2, quarter, -1)
        given = swap(pick(grad_e, 1 - c, 1).astype(BF), "c")
        return grad_e, given

    projected = values_call(1 - core, modulated, weight_got, projected)

    forward = by_core(along("x", 1), along("z", 1))
    back = by_core(along("x", 3), along("z", 3))
    chunk, (grad_e, given_e) = ring_reduce(
        lambda d: cut(blocks_w, d), 2, forward, back, embed_gradient
    )
    grad_e = (pick(grad_e, c, 1) + given_e.astype(F32)).astype(BF).reshape(4, 4, 96, -1)
    chunk_e = add_up(
        direct_pieces(lambda d: cut(grad_e, d), lambda d: by_core(along("x", d), along("z", d)))
    )
    chunk = jnp.concatenate([chunk.astype(BF), chunk_e.astype(BF)], axis=-1)

    def second(d):
        return pick(chunk, jnp.where(c == 0, z_at(d), x_at(d)), 0)

    rows = add_up(direct_pieces(second, lambda d: by_core(along("z", d), along("x", d))))
    rows = rows.reshape(4, 24, -1)
    last = direct_pieces(lambda d: pick(rows, (pos["y"] + d) % 4, 0), lambda d: along("y", d))
    grad_value = add_up([piece[:, :cols] for piece in last])
    grad_embed = add_up([piece[:, cols:] for piece in last])
    return (projected.reshape(value_cotangent.shape), grad_value, grad_embed)


def solution(mesh):
    sub = Mesh(mesh.devices.reshape(SIZES), AXES)
    enc, fsdp = ("zl", "c"), ("zh", "x", "y")
    in_specs = (
        P(None, enc, fsdp, None),
        P(),
        P(),
        P(),
        P(),
        P(),
        P(fsdp, None),
        P(fsdp, None),
        P(fsdp, None),
        P(fsdp, None),
        P(fsdp, enc, None, None),
    )
    out_specs = (P(fsdp, enc, None, None), P(enc + fsdp, None), P(enc + fsdp, None))
    return jax.shard_map(local, mesh=sub, in_specs=in_specs, out_specs=out_specs, check_vma=False)
```
